32 devices in a mesh: replica: 4 (over x, core), fsdp: 4 (over z), tensor: 2 (over y).
Axes of the slice: x: 2, y: 2, z: 4, core: 2. Of those that a mesh axis runs over, the one named last changes fastest.
Arguments:
- pseudo_grad: bfloat16 [4, 3072, 18432], P('replica', 'fsdp', 'tensor'), may hold values from -6 to 6
- compensation: float32 [4, 3072, 18432], P('replica', 'fsdp', 'tensor'), may hold values from -6 to 6
- params: float32 [3072, 18432], P(('fsdp', 'replica'), 'tensor'), may hold values from -6 to 6
- momentum: float32 [3072, 18432], P(('fsdp', 'replica'), 'tensor'), may hold values from -6 to 6
- probe: bfloat16 [256, 18432], P('fsdp', 'tensor'), may hold values from -0.046875 to 0.046875
Outputs:
- new_params: float32 [3072, 18432], P(('fsdp', 'replica'), 'tensor')
- new_momentum: float32 [3072, 18432], P(('fsdp', 'replica'), 'tensor')
- probe_out: bfloat16 [256, 3072], P('tensor', 'fsdp')
The draws below stay inside these ranges and needn't reach their ends.
All inputs are finite; a program needn't handle non-finite values.
Results may differ from the reference program's by a relative error of at most 0.014.
Values may be sent and summed in bfloat16 or wider, within the bound.
A program may use at most 128 MiB of HBM per device.

```python
import jax
import jax.numpy as jnp
from jax import lax

D = 3072
FW = 18432
PROBE = 256
N_REPLICA = 4


def spiked(entries, rng, source, target, shards_of, factor):
    def block_of(dim):
        return (jnp.arange(entries.shape[dim]) // (entries.shape[dim] // shards_of)).reshape((-1,) + (1,) * (entries.ndim - 1 - dim))

    one_side = jax.random.permutation(rng, shards_of)[block_of(target)]
    far = (block_of(target) + shards_of // 2) % shards_of
    return jnp.where((block_of(source) == one_side) | (block_of(source) == far), factor * entries, entries)


def steps_of(rng, dims, pieces, smallest, top_value):
    def one(position, parts):
        draws = jax.random.uniform(jax.random.fold_in(jax.random.fold_in(rng, 6), position), (parts,), jnp.float32, smallest / len(pieces), top_value / len(pieces))
        return jnp.repeat(jnp.exp(draws), dims[position] // parts).reshape((-1,) + (1,) * (len(dims) - position - 1))

    factor_of = one(*pieces[0])
    for cut in pieces[1:]:
        factor_of = factor_of * one(*cut)
    return factor_of


def noise(own_key, extent, spread, bound, shards=(), held_as=jnp.bfloat16):
    drawn = spread * jax.random.normal(own_key, extent, jnp.float32)
    if shards:
        drawn = drawn * steps_of(own_key, extent, shards, -0.22, 0.18)
    return jnp.clip(drawn, -bound, bound).astype(held_as)


def heavy_noise(rng, dims, scale, most, shards, heavy, dtype=jnp.bfloat16):
    result = scale * jax.random.normal(rng, dims, jnp.float32)
    if shards:
        result = result * steps_of(rng, dims, shards, -0.22, 0.18)
    return jnp.clip(spiked(result, jax.random.fold_in(rng, 3), *heavy), -most, most).astype(dtype)


def setup_inputs(seed: int = 0) -> dict:
    key_list = jax.random.split(jax.random.key(seed), 6)
    pseudo_grad = heavy_noise(key_list[0], (N_REPLICA, D, FW), 1.0, 6.0, ((0, 4), (1, 4), (2, 2)), (0, 1, 4, 2.0))
    compensation = noise(key_list[1], (N_REPLICA, D, FW), 1.0, 6.0, ((0, 4), (1, 4), (2, 2)), jnp.float32)
    params = noise(key_list[2], (D, FW), 1.0, 6.0, ((0, 16), (1, 2)), jnp.float32)
    momentum = noise(key_list[3], (D, FW), 1.0, 6.0, ((0, 16), (1, 2)), jnp.float32)
    probe = noise(key_list[4], (PROBE, FW), FW ** -0.5, 0.046875, ((0, 4), (1, 2)))
    return dict(pseudo_grad=pseudo_grad, compensation=compensation, params=params, momentum=momentum, probe=probe)


outer_rate = 0.7
nesterov = 0.9


def reference(pseudo_grad, compensation, params, momentum, probe):
    def accumulate(summed, pair):
        grads, carried = pair
        outgoing = (grads.astype(jnp.float32) + carried).astype(jnp.bfloat16)
        outgoing = lax.optimization_barrier(outgoing)
        return summed + outgoing.astype(jnp.float32), None

    start = jnp.zeros(params.shape, jnp.float32)
    summed, _ = lax.scan(accumulate, start, (pseudo_grad, compensation))
    average = summed / N_REPLICA
    new_momentum = nesterov * momentum + average
    new_params = params - outer_rate * (average + nesterov * new_momentum)
    weights = new_params.astype(jnp.bfloat16)
    probe_out = lax.dot_general(probe, weights, (((1,), (1,)), ((), ())), preferred_element_type=jnp.float32)
    return new_params, new_momentum, probe_out.astype(jnp.bfloat16)
```

```python
import functools

import jax
import jax.numpy as jnp
from jax import lax
from jax.experimental import pallas as pl
from jax.experimental.pallas import tpu as pltpu
from jax.sharding import PartitionSpec as P

outer_rate = 0.7
nesterov = 0.9
f32, bf16 = jnp.float32, jnp.bfloat16
MESH = pl.DeviceIdType.MESH

SLOTS = 4


def mean(summed, n):
    return summed * (1.0 / n) if n & (n - 1) == 0 else summed / n


def kernel(sizes, grad, carried, params, momentum, probe, *refs):
    n, n_fsdp, splits, rows, columns, tile, height = sizes
    (
        new_params, new_momentum, probe_out,
        grad_in, carried_in, give, got, part, arrived, own, probes, total,
        half_out, half_in, blocks,
        grad_sem, carried_sem, state_sem,
        give_send, give_recv, part_send, part_recv,
        fetch_send, fetch_recv, share_send, share_recv,
        half_send, half_recv, block_send, block_recv,
    ) = refs
    chips = n // 2
    tiles = columns // tile
    items = chips * tiles
    me = lax.axis_index("replica")
    chip, core = lax.div(me, 2), lax.rem(me, 2)
    here = lax.axis_index("fsdp")
    mine = lax.axis_index("tensor")
    mate = {"replica": chip * 2 + 1 - core}
    across = [{"replica": lax.rem(chip + s, chips) * 2 + core} for s in range(1, chips)]
    along = [{"fsdp": lax.rem(here + s, n_fsdp)} for s in range(1, n_fsdp)]
    beside = [{"tensor": lax.rem(mine + s, splits)} for s in range(1, splits)]

    def remote(src, dst, send, recv, device):
        return pltpu.make_async_remote_copy(
            src_ref=src, dst_ref=dst, send_sem=send, recv_sem=recv,
            device_id=device, device_id_type=MESH,
        )

    def fetch(k):
        there = lax.rem(chip + 1 + lax.div(k, tiles), chips)
        slot = lax.rem(k, SLOTS)
        at = (
            0,
            pl.ds(pl.multiple_of(there * (2 * rows), 2 * rows), 2 * rows),
            pl.ds(pl.multiple_of(lax.rem(k, tiles) * tile, tile), tile),
        )
        return (
            pltpu.make_async_copy(grad.at[at], grad_in.at[slot], grad_sem.at[slot]),
            pltpu.make_async_copy(carried.at[at], carried_in.at[slot], carried_sem.at[slot]),
        )

    def start_fetch(k):
        for copy in fetch(k):
            copy.start()

    def outgoing(k, which):
        slot = lax.rem(k, SLOTS)
        at = pl.ds(pl.multiple_of(which * rows, rows), rows)
        return grad_in[slot, at, :].astype(f32) + carried_in[slot, at, :]

    def give_copy(k):
        slot = lax.rem(k, SLOTS)
        return remote(give.at[slot], got.at[k], give_send.at[slot], give_recv.at[k], mate)

    def part_copy(k, step):
        return remote(part.at[k], arrived.at[k], part_send.at[k], part_recv.at[k], across[step])

    def first(k):
        for copy in fetch(k):
            copy.wait()

        @pl.when(k >= SLOTS)
        def _():
            give_copy(k - SLOTS).wait_send()

        give[lax.rem(k, SLOTS)] = outgoing(k, 1 - core).astype(bf16)
        give_copy(k).start()

    def second(k, step):
        give_copy(k).wait_recv()
        summed = outgoing(k, core) + got[k].astype(f32)
        if step < chips - 1:
            part[k] = summed.astype(bf16)
            part_copy(k, step).start()
        else:
            own[k - step * tiles] = summed

        @pl.when(k + SLOTS < items)
        def _():
            start_fetch(k + SLOTS)

    for k in range(min(SLOTS, items)):
        start_fetch(jnp.int32(k))

    barrier = pltpu.get_barrier_semaphore()
    peers = [mate] + across + along + beside
    for peer in peers:
        pl.semaphore_signal(barrier, inc=1, device_id=peer, device_id_type=MESH)
    pl.semaphore_wait(barrier, len(peers))

    half = height // 2
    half_at = lambda place: pl.ds(pl.multiple_of(place * height + core * half, half), half)
    own_half = pl.ds(pl.multiple_of(core * half, half), half)
    own_probe = pltpu.make_async_copy(
        probe, probes.at[pl.ds(pl.multiple_of(here * height, height), height), :], state_sem.at[2]
    )

    def probe_copy(step):
        return remote(
            probe.at[own_half, :], probes.at[half_at(here), :],
            fetch_send.at[step], fetch_recv.at[step], along[step],
        )

    def share_copy(step):
        place = half_at(lax.rem(here + n_fsdp - 1 - step, n_fsdp))
        return remote(
            probes.at[place, :], probes.at[place, :],
            share_send.at[step], share_recv.at[step], mate,
        )

    first(jnp.int32(0))
    state = (
        pltpu.make_async_copy(params, new_params, state_sem.at[0]),
        pltpu.make_async_copy(momentum, new_momentum, state_sem.at[1]),
    )
    for step in range(chips):
        last = step == chips - 1

        def body(k, carry, step=step):
            first(k)
            second(k - 1, step)
            return carry

        lax.fori_loop(step * tiles + 1, (step + 1) * tiles + (0 if last else 1), body, 0)
        if step == 0:
            own_probe.start()
            for i in range(n_fsdp - 1):
                probe_copy(i).start()
            for copy in state:
                copy.start()
    second(jnp.int32(items - 1), chips - 1)

    for copy in state:
        copy.wait()
    own_probe.wait()
    total[...] = jnp.zeros_like(total)

    def update(t):
        at = pl.ds(pl.multiple_of(t * tile, tile), tile)
        summed = own[t]
        for step in range(chips - 1):
            k = step * tiles + t
            part_copy(k, step).wait_recv()
            summed += arrived[k].astype(f32)
        average = mean(summed, n)
        moved = nesterov * new_momentum[:, at] + average
        updated = new_params[:, at] - outer_rate * (average + nesterov * moved)
        new_momentum[:, at] = moved
        new_params[:, at] = updated
        return updated.astype(bf16)

    def product(t, weights):
        at = pl.ds(pl.multiple_of(t * tile, tile), tile)
        total[...] += lax.dot_general(
            probes[:, at], weights, (((1,), (1,)), ((), ())), preferred_element_type=f32
        )

    early = max(1, (2 * tiles) // 3)

    def before(t, carry):
        got[t] = update(t)
        return carry

    lax.fori_loop(0, early, before, 0)
    for i in range(n_fsdp - 1):
        probe_copy(i).wait_recv()
        share_copy(i).start()
    for i in range(n_fsdp - 1):
        share_copy(i).wait_recv()

    def backlog(t, carry):
        product(t, got[t])
        return carry

    lax.fori_loop(0, early, backlog, 0)

    def after(t, carry):
        product(t, update(t))
        return carry

    lax.fori_loop(early, tiles, after, 0)

    batch = half_out.shape[1]
    piece = lambda which: total[pl.ds(pl.multiple_of(which * batch, batch), batch), :]
    halves = []
    for i in range(splits - 1):
        half_out[i] = piece(lax.rem(mine + 1 + i, splits)).astype(bf16)
        copy = remote(half_out.at[i], half_in.at[i], half_send.at[i], half_recv.at[i], beside[i])
        copy.start()
        halves.append(copy)
    column_part = piece(mine)
    for i, copy in enumerate(halves):
        copy.wait_recv()
        column_part += half_in[i].astype(f32)
    blocks[me] = column_part.astype(bf16)

    def block_copy(which, slot, device):
        return remote(
            blocks.at[which], blocks.at[which], block_send.at[slot], block_recv.at[slot], device
        )

    sends = [block_copy(me, s, across[s]) for s in range(chips - 1)]
    sends.append(block_copy(me, chips - 1, mate))
    for copy in sends:
        copy.start()
    for s in range(chips - 1):
        source = lax.rem(chip + chips - 1 - s, chips) * 2 + core
        sends[s].wait_recv()
        copy = block_copy(source, chips + s, mate)
        copy.start()
        sends.append(copy)
    for copy in sends[chips - 1 :]:
        copy.wait_recv()
    probe_out[...] = jnp.concatenate([blocks[r] for r in range(n)], axis=1)

    for copy in halves + sends:
        copy.wait_send()
    for k in range(max(0, items - SLOTS), items):
        give_copy(jnp.int32(k)).wait_send()
    for step in range(chips - 1):
        def drain(k, carry, step=step):
            part_copy(k, step).wait_send()
            return carry

        lax.fori_loop(step * tiles, (step + 1) * tiles, drain, 0)
    for i in range(n_fsdp - 1):
        probe_copy(i).wait_send()
        share_copy(i).wait_send()


def per_device(pseudo_grad, compensation, params, momentum, probe):
    n = lax.axis_size("replica")
    n_fsdp = lax.axis_size("fsdp")
    splits = lax.axis_size("tensor")
    chips = n // 2
    rows, columns = params.shape
    height = probe.shape[0]
    tile = 512 if columns % 512 == 0 else 128
    tiles = columns // tile
    batch = n_fsdp * height
    dma = pltpu.SemaphoreType.DMA
    anywhere = pl.BlockSpec(memory_space=pl.ANY)
    vmem = pl.BlockSpec(memory_space=pltpu.VMEM)
    links = max(1, n_fsdp - 1)
    return pl.pallas_call(
        functools.partial(kernel, (n, n_fsdp, splits, rows, columns, tile, height)),
        out_shape=(
            pltpu.VMEM((rows, columns), f32),
            pltpu.VMEM((rows, columns), f32),
            jax.ShapeDtypeStruct((batch // splits, n * rows), bf16),
        ),
        in_specs=[anywhere] * 5,
        out_specs=[vmem] * 3,
        scratch_shapes=[
            pltpu.VMEM((SLOTS, 2 * rows, tile), bf16),
            pltpu.VMEM((SLOTS, 2 * rows, tile), f32),
            pltpu.VMEM((SLOTS, rows, tile), bf16),
            pltpu.VMEM((chips * tiles, rows, tile), bf16),
            pltpu.VMEM(((chips - 1) * tiles, rows, tile), bf16),
            pltpu.VMEM(((chips - 1) * tiles, rows, tile), bf16),
            pltpu.VMEM((tiles, rows, tile), f32),
            pltpu.VMEM((batch, columns), bf16),
            pltpu.VMEM((batch, rows), f32),
            pltpu.VMEM((splits - 1, batch // splits, rows), bf16),
            pltpu.VMEM((splits - 1, batch // splits, rows), bf16),
            pltpu.VMEM((n, batch // splits, rows), bf16),
            dma((SLOTS,)), dma((SLOTS,)), dma((3,)),
            dma((SLOTS,)), dma((chips * tiles,)),
            dma(((chips - 1) * tiles,)), dma(((chips - 1) * tiles,)),
            dma((links,)), dma((links,)), dma((links,)), dma((links,)),
            dma((splits - 1,)), dma((splits - 1,)),
            dma((n - 1,)), dma((n - 1,)),
        ],
        compiler_params=pltpu.CompilerParams(
            collective_id=0, has_side_effects=True, vmem_limit_bytes=46 * 1024 * 1024
        ),
    )(pseudo_grad, compensation, params, momentum, probe)


def solution(mesh):
    in_specs = (
        P("replica", "fsdp", "tensor"),
        P("replica", "fsdp", "tensor"),
        P(("fsdp", "replica"), "tensor"),
        P(("fsdp", "replica"), "tensor"),
        P("fsdp", "tensor"),
    )
    out_specs = (
        P(("fsdp", "replica"), "tensor"),
        P(("fsdp", "replica"), "tensor"),
        P("tensor", "fsdp"),
    )
    return jax.shard_map(
        per_device, mesh=mesh, in_specs=in_specs, out_specs=out_specs, check_vma=False
    )
```

```python
import functools

import jax
import jax.numpy as jnp
from jax import lax
from jax.experimental import pallas as pl
from jax.experimental.pallas import tpu as pltpu
from jax.sharding import PartitionSpec as P

outer_rate = 0.7
nesterov = 0.9
f32, bf16 = jnp.float32, jnp.bfloat16
MESH = pl.DeviceIdType.MESH

SLOTS = 4
AHEAD = 6
OPENING = 2
BUFFERS = 11


def mean(summed, n):
    return summed * (1.0 / n) if n & (n - 1) == 0 else summed / n


def segments_of(rows, columns):
    fit = lambda width: width if columns % width == 0 else 128
    late = 32 if rows >= 64 else rows
    if late == rows:
        return [(0, rows, fit(512))]
    return [(0, rows - late, fit(1024)), (rows - late, late, fit(1024))]


def kernel(sizes, grad, carried, params, momentum, probe, *refs):
    n, n_fsdp, splits, rows, columns, height, segments = sizes
    refs = list(refs)
    take = lambda count: [refs.pop(0) for _ in range(count)]
    new_params, new_momentum, gathered = take(3)
    buffers = [take(BUFFERS) for _ in segments]
    probes, late_out, late_in = take(3)
    early_out, early_in = take(2) if len(segments) > 1 else (None, None)
    (
        state_sem, right_send, left_send, fetch_recv, share_send, share_recv,
        late_send, late_recv, early_send, early_recv, block_send, block_recv,
    ) = refs
    chips = n // 2
    me = lax.axis_index("replica")
    chip, core = lax.div(me, 2), lax.rem(me, 2)
    here = lax.axis_index("fsdp")
    mine = lax.axis_index("tensor")
    mate = {"replica": chip * 2 + 1 - core}
    across = [{"replica": lax.rem(chip + s, chips) * 2 + core} for s in range(1, chips)]
    beside = [{"tensor": lax.rem(mine + s, splits)} for s in range(1, splits)]
    multiple = lambda index, size: pl.ds(pl.multiple_of(index * size, size), size)

    def remote(src, dst, send, recv, device):
        return pltpu.make_async_remote_copy(
            src_ref=src, dst_ref=dst, send_sem=send, recv_sem=recv,
            device_id=device, device_id_type=MESH,
        )

    class Segment:
        def __init__(self, spec, parts, held):
            self.row, self.rows, self.tile = spec
            (
                self.grad_in, self.carried_in, self.give, self.got, self.part, self.arrived, self.own,
                self.total, self.in_sem, self.give_sem, self.part_sem,
            ) = parts
            self.tiles = columns // self.tile
            self.items = chips * self.tiles
            self.held = held

        def fetch(self, k):
            there = lax.rem(chip + 1 + lax.div(k, self.tiles), chips)
            slot = lax.rem(k, SLOTS)
            copies = []
            for which in range(2):
                start = (there * 2 + which) * rows + self.row
                at = (0, pl.ds(pl.multiple_of(start, 16), self.rows), multiple(lax.rem(k, self.tiles), self.tile))
                for i, (array, into) in enumerate(((grad, self.grad_in), (carried, self.carried_in))):
                    copies.append(
                        pltpu.make_async_copy(
                            array.at[at], into.at[slot, which], self.in_sem.at[slot, 2 * which + i]
                        )
                    )
            return copies

        def start_fetch(self, k):
            for copy in self.fetch(k):
                copy.start()

        def outgoing(self, k, which):
            slot = lax.rem(k, SLOTS)
            return self.grad_in[slot, which].astype(f32) + self.carried_in[slot, which]

        def give_copy(self, k):
            slot = lax.rem(k, SLOTS)
            return remote(self.give.at[slot], self.got.at[k], self.give_sem.at[slot], self.give_sem.at[SLOTS + k], mate)

        def part_copy(self, k, step):
            return remote(
                self.part.at[k], self.arrived.at[k], self.part_sem.at[0, k], self.part_sem.at[1, k], across[step]
            )

        def first(self, k, send=True):
            for copy in self.fetch(k):
                copy.wait()

            @pl.when(k >= SLOTS)
            def _():
                self.give_copy(k - SLOTS).wait_send()

            self.give[lax.rem(k, SLOTS)] = self.outgoing(k, 1 - core).astype(bf16)
            if send:
                self.give_copy(k).start()

        def second(self, k, step, now=False):
            summed = self.outgoing(k, core)
            self.give_copy(k).wait_recv()
            summed += self.got[k].astype(f32)
            if step < chips - 1:
                self.part[k] = summed.astype(bf16)
                if now or not self.held:
                    self.part_copy(k, step).start()
            else:
                self.own[k - step * self.tiles] = summed

            @pl.when(k + SLOTS < self.items)
            def _():
                self.start_fetch(k + SLOTS)

        def run(self, step, begun=0):
            start, end = step * self.tiles + begun, (step + 1) * self.tiles
            if start >= end:
                return
            self.first(jnp.int32(start))

            def body(k, carry):
                self.first(k)
                self.second(k - 1, step)
                return carry

            lax.fori_loop(start + 1, end, body, 0)
            self.second(jnp.int32(end - 1), step)

        def update(self, t):
            at = (pl.ds(self.row, self.rows), multiple(t, self.tile))
            summed = self.own[t]
            for step in range(chips - 1):
                k = step * self.tiles + t
                self.part_copy(k, step).wait_recv()
                summed += self.arrived[k].astype(f32)
            average = mean(summed, n)
            moved = nesterov * new_momentum[at] + average
            updated = new_params[at] - outer_rate * (average + nesterov * moved)
            new_momentum[at] = moved
            new_params[at] = updated
            return updated.astype(bf16)

        def product(self, t, weights):
            self.total[...] += lax.dot_general(
                weights, probes[:, multiple(t, self.tile)], (((1,), (1,)), ((), ())),
                preferred_element_type=f32,
            )

        def drain(self):
            for k in range(max(0, self.items - SLOTS), self.items):
                self.give_copy(jnp.int32(k)).wait_send()
            for step in range(chips - 1):
                def body(k, carry, step=step):
                    self.part_copy(k, step).wait_send()
                    return carry

                lax.fori_loop(step * self.tiles, (step + 1) * self.tiles, body, 0)

    held = len(segments) > 1 and chips == 2
    parts = [Segment(s, b, held and i == 1) for i, (s, b) in enumerate(zip(segments, buffers))]
    main, late = parts[0], parts[-1]

    for k in range(min(OPENING, late.tiles)):
        late.start_fetch(jnp.int32(k))
    barrier = pltpu.get_barrier_semaphore()
    others = [(r, t) for r in range(n) for t in range(splits) if r or t]
    other = lambda r, t: {"replica": lax.rem(me + r, n), "tensor": lax.rem(mine + t, splits)}
    near = [mate] + across + beside if len(segments) > 1 else [other(r, t) for r, t in others]
    for peer in near:
        pl.semaphore_signal(barrier, inc=1, device_id=peer, device_id_type=MESH)
    is_right, is_left = here + 1 < n_fsdp, here >= 1
    right, left = {"fsdp": here + 1}, {"fsdp": here - 1}

    @pl.when(is_right)
    def _():
        pl.semaphore_signal(barrier, inc=1, device_id=right, device_id_type=MESH)

    @pl.when(is_left)
    def _():
        pl.semaphore_signal(barrier, inc=1, device_id=left, device_id_type=MESH)

    opening = min(OPENING, late.tiles)
    late.first(jnp.int32(0), send=False)
    if main is not late:
        main.start_fetch(jnp.int32(0))
    pl.semaphore_wait(barrier, len(near) + is_right.astype(jnp.int32) + is_left.astype(jnp.int32))

    half = height // 2
    half_at = lambda place: pl.ds(pl.multiple_of(place * height + core * half, half), half)
    own_probe = pltpu.make_async_copy(probe, probes.at[multiple(here, height), :], state_sem.at[2])

    def right_copy(s):
        block = here - s + 1
        src = probe.at[multiple(core, half), :] if s == 1 else probes.at[half_at(block), :]
        return remote(src, probes.at[half_at(block), :], right_send.at[s - 1], fetch_recv.at[block], right)

    def left_copy(s):
        block = here + s - 1
        src = probe.at[multiple(core, half), :] if s == 1 else probes.at[half_at(block), :]
        return remote(src, probes.at[half_at(block), :], left_send.at[s - 1], fetch_recv.at[block], left)

    def share_copy(block):
        place = half_at(block)
        return remote(probes.at[place, :], probes.at[place, :], share_send.at[block], share_recv.at[block], mate)

    def relay(s, act):
        @pl.when(is_right & (here - s + 1 >= 0))
        def _():
            act(right_copy(s))

        @pl.when(is_left & (here + s - 1 < n_fsdp))
        def _():
            act(left_copy(s))

    start = lambda copy: copy.start()
    wait_send = lambda copy: copy.wait_send()
    wait_recv = lambda copy: copy.wait_recv()

    def landed(s, act):
        @pl.when(here - s >= 0)
        def _():
            act(here - s, right_copy)

        @pl.when(here + s < n_fsdp)
        def _():
            act(here + s, left_copy)

    def land(s):
        def act(block, _):
            place = half_at(block)
            remote(
                probes.at[place, :], probes.at[place, :], right_send.at[0], fetch_recv.at[block], mate
            ).wait_recv()
            share_copy(block).start()

        landed(s, act)
        if s + 1 < n_fsdp:
            relay(s + 1, start)

    late.give_copy(jnp.int32(0)).start()
    for k in range(1, opening):
        late.first(jnp.int32(k))
    for k in range(opening):
        late.second(jnp.int32(k), 0, now=True)
    if n_fsdp > 1:
        relay(1, start)
    own_probe.start()
    if main is not late:
        for k in range(1, min(SLOTS, main.items)):
            main.start_fetch(jnp.int32(k))
    for k in range(opening, min(SLOTS, late.items)):
        late.start_fetch(jnp.int32(k))
    state = (
        pltpu.make_async_copy(params, new_params, state_sem.at[0]),
        pltpu.make_async_copy(momentum, new_momentum, state_sem.at[1]),
    )
    for step in range(chips - 1):
        for i, part in enumerate(parts):
            part.run(step, begun=opening if step == 0 and part is late else 0)
    for copy in state:
        copy.start()
    if n_fsdp > 1:
        land(1)
    for part in parts:
        part.run(chips - 1)
    if n_fsdp > 2:
        land(2)
    for copy in state:
        copy.wait()
    own_probe.wait()
    for part in parts:
        part.total[...] = jnp.zeros_like(part.total)

    first_products = max(1, (2 * main.tiles) // 3)

    def before(t, carry):
        main.got[t] = main.update(t)
        return carry

    lax.fori_loop(0, first_products, before, 0)
    for s in range(3, n_fsdp):
        land(s)
    for s in range(1, n_fsdp):
        landed(s, lambda block, _: share_copy(block).wait_recv())

    def backlog(t, carry):
        main.product(t, main.got[t])
        return carry

    lax.fori_loop(0, first_products, backlog, 0)

    def after(part):
        def body(t, carry):
            part.product(t, part.update(t))
            return carry

        return body

    batch = n_fsdp * height
    piece = batch // splits
    copies = []
    if len(parts) == 1:
        lax.fori_loop(first_products, main.tiles, after(main), 0)
    else:
        turn = max(first_products, main.tiles - 2)
        lax.fori_loop(first_products, turn, after(main), 0)
        lead = min(AHEAD, late.tiles - opening)
        if held:
            for k in range(opening, opening + lead):
                late.part_copy(jnp.int32(k), 0).start()
        lax.fori_loop(turn, main.tiles, after(main), 0)

        halves = []
        for i in range(splits - 1):
            early_out[i] = main.total[:, multiple(lax.rem(mine + 1 + i, splits), piece)].astype(bf16)
            copy = remote(early_out.at[i], early_in.at[i], early_send.at[i], early_recv.at[i], beside[i])
            copy.start()
            halves.append(copy)
        copies += halves

        def late_step(t, carry):
            if held:
                @pl.when(t + opening + lead < late.tiles)
                def _():
                    late.part_copy(t + opening + lead, 0).start()

            return after(late)(t, carry)

        middle = min(3, late.tiles)
        lax.fori_loop(0, middle, late_step, 0)
        summed = main.total[:, multiple(mine, piece)]
        for i, copy in enumerate(halves):
            copy.wait_recv()
            summed += early_in[i].astype(f32)
        block_at = lambda which: pl.ds(pl.multiple_of(which * rows, 16), main.rows)
        gathered[block_at(me), :] = summed.astype(bf16)

        def block_copy(which, slot, device):
            ref = gathered.at[block_at(which), :]
            return remote(ref, ref, block_send.at[slot], block_recv.at[slot], device)

        sends = [block_copy(me, s, across[s]) for s in range(chips - 1)]
        sends.append(block_copy(me, chips - 1, mate))
        for copy in sends:
            copy.start()
        lax.fori_loop(middle, late.tiles, late_step, 0)

    for t in range(splits):
        late_out[t] = late.total[:, multiple(lax.rem(mine + t, splits), piece)].astype(bf16)
    messages = [
        remote(
            late_out.at[t], late_in.at[r * splits + t],
            late_send.at[r * splits + t], late_recv.at[r * splits + t], other(r, t),
        )
        for r, t in others
    ]
    for copy in messages:
        copy.start()
    copies += messages
    if len(parts) > 1:
        for s in range(chips - 1):
            source = lax.rem(chip + chips - 1 - s, chips) * 2 + core
            sends[s].wait_recv()
            copy = block_copy(source, chips + s, mate)
            copy.start()
            sends.append(copy)
        copies += sends
    for part in parts:
        part.drain()
    for s in range(1, n_fsdp):
        relay(s, wait_send)
        landed(s, lambda block, _: share_copy(block).wait_send())
    for copy in messages:
        copy.wait_recv()
    for r in range(n):
        summed = jnp.zeros((late.rows, piece), f32)
        for t in range(splits):
            summed += (late_in[r * splits + t] if r or t else late_out[0]).astype(f32)
        source = lax.rem(me + n - r, n)
        gathered[pl.ds(pl.multiple_of(source * rows + late.row, 16), late.rows), :] = summed.astype(bf16)
    if len(parts) > 1:
        for copy in sends[chips - 1 :]:
            copy.wait_recv()
    for copy in copies:
        copy.wait_send()


def writer(params_in, momentum_in, gathered, params_out, momentum_out, probe_out, turned, sem):
    copies = (
        pltpu.make_async_copy(params_in, params_out, sem.at[0]),
        pltpu.make_async_copy(momentum_in, momentum_out, sem.at[1]),
    )
    for copy in copies:
        copy.start()
    turned[...] = gathered[...].astype(f32).T.astype(bf16)
    last = pltpu.make_async_copy(turned, probe_out, sem.at[2])
    last.start()
    for copy in (*copies, last):
        copy.wait()


def per_device(pseudo_grad, compensation, params, momentum, probe):
    n = lax.axis_size("replica")
    n_fsdp = lax.axis_size("fsdp")
    splits = lax.axis_size("tensor")
    chips = n // 2
    rows, columns = params.shape
    height = probe.shape[0]
    batch = n_fsdp * height
    piece = batch // splits
    segments = segments_of(rows, columns)
    dma = pltpu.SemaphoreType.DMA
    anywhere = pl.BlockSpec(memory_space=pl.ANY)
    vmem = pl.BlockSpec(memory_space=pltpu.VMEM)
    scratch = []
    for _, high, tile in segments:
        tiles = columns // tile
        sends = max(1, chips - 1) * tiles
        scratch += [
            pltpu.VMEM((SLOTS, 2, high, tile), bf16),
            pltpu.VMEM((SLOTS, 2, high, tile), f32),
            pltpu.VMEM((SLOTS, high, tile), bf16),
            pltpu.VMEM((chips * tiles, high, tile), bf16),
            pltpu.VMEM((sends, high, tile), bf16),
            pltpu.VMEM((sends, high, tile), bf16),
            pltpu.VMEM((tiles, high, tile), f32),
            pltpu.VMEM((high, batch), f32),
            dma((SLOTS, 4)),
            dma((SLOTS + chips * tiles,)),
            dma((2, sends)),
        ]
    _, late, _ = segments[-1]
    early = segments[0][1]
    scratch += [
        pltpu.VMEM((batch, columns), bf16),
        pltpu.VMEM((splits, late, piece), bf16),
        pltpu.VMEM((n * splits, late, piece), bf16),
    ]
    if len(segments) > 1:
        scratch += [pltpu.VMEM((max(1, splits - 1), early, piece), bf16)] * 2
    links = max(1, n_fsdp)
    scratch += [dma((3,))] + [dma((links,))] * 5 + [dma((n * splits,))] * 2 + [dma((splits,))] * 2 + [dma((n,))] * 2
    full = pltpu.VMEM((rows, columns), f32)
    new_params, new_momentum, gathered = pl.pallas_call(
        functools.partial(kernel, (n, n_fsdp, splits, rows, columns, height, segments)),
        out_shape=(full, full, pltpu.VMEM((n * rows, piece), bf16)),
        in_specs=[anywhere] * 5,
        out_specs=[vmem] * 3,
        scratch_shapes=scratch,
        compiler_params=pltpu.CompilerParams(
            collective_id=0, has_side_effects=True, vmem_limit_bytes=46 * 1024 * 1024
        ),
    )(pseudo_grad, compensation, params, momentum, probe)
    full = jax.ShapeDtypeStruct((rows, columns), f32)
    return pl.pallas_call(
        writer,
        out_shape=(full, full, jax.ShapeDtypeStruct((piece, n * rows), bf16)),
        in_specs=[vmem] * 3,
        out_specs=[anywhere] * 3,
        scratch_shapes=[pltpu.VMEM((piece, n * rows), bf16), dma((3,))],
        compiler_params=pltpu.CompilerParams(vmem_limit_bytes=8 * 1024 * 1024),
    )(*(pltpu.with_memory_space_constraint(x, pltpu.VMEM) for x in (new_params, new_momentum, gathered)))


def solution(mesh):
    in_specs = (
        P("replica", "fsdp", "tensor"),
        P("replica", "fsdp", "tensor"),
        P(("fsdp", "replica"), "tensor"),
        P(("fsdp", "replica"), "tensor"),
        P("fsdp", "tensor"),
    )
    out_specs = (
        P(("fsdp", "replica"), "tensor"),
        P(("fsdp", "replica"), "tensor"),
        P("tensor", "fsdp"),
    )
    return jax.shard_map(
        per_device, mesh=mesh, in_specs=in_specs, out_specs=out_specs, check_vma=False
    )
```

```python
import functools

import jax
import jax.numpy as jnp
from jax import lax
from jax.experimental import pallas as pl
from jax.experimental.pallas import tpu as pltpu
from jax.sharding import PartitionSpec as P

outer_rate = 0.7
nesterov = 0.9
f32, bf16 = jnp.float32, jnp.bfloat16
MESH = pl.DeviceIdType.MESH

SLOTS = 3
AHEAD = 6
OPENING = 3
BUFFERS = 11


def mean(summed, n):
    return summed * (1.0 / n) if n & (n - 1) == 0 else summed / n


def segments_of(rows, columns):
    fit = lambda width: width if columns % width == 0 else 128
    late = 32 if rows >= 64 else rows
    if late == rows:
        return [(0, rows, fit(512))]
    return [(0, rows - late, fit(1536)), (rows - late, late, fit(1024))]


def kernel(sizes, grad, carried, params, momentum, probe, *refs):
    n, n_fsdp, splits, rows, columns, height, segments = sizes
    refs = list(refs)
    take = lambda count: [refs.pop(0) for _ in range(count)]
    new_params, new_momentum, gathered = take(3)
    buffers = [take(BUFFERS) for _ in segments]
    probes, late_out, late_in = take(3)
    early_out, early_in = take(2) if len(segments) > 1 else (None, None)
    (
        state_sem, right_send, left_send, fetch_recv, share_send, share_recv,
        late_send, late_recv, early_send, early_recv, block_send, block_recv,
    ) = refs
    chips = n // 2
    me = lax.axis_index("replica")
    chip, core = lax.div(me, 2), lax.rem(me, 2)
    here = lax.axis_index("fsdp")
    mine = lax.axis_index("tensor")
    mate = {"replica": chip * 2 + 1 - core}
    across = [{"replica": lax.rem(chip + s, chips) * 2 + core} for s in range(1, chips)]
    beside = [{"tensor": lax.rem(mine + s, splits)} for s in range(1, splits)]
    multiple = lambda index, size: pl.ds(pl.multiple_of(index * size, size), size)

    def remote(src, dst, send, recv, device):
        return pltpu.make_async_remote_copy(
            src_ref=src, dst_ref=dst, send_sem=send, recv_sem=recv,
            device_id=device, device_id_type=MESH,
        )

    class Segment:
        def __init__(self, spec, parts, held):
            self.row, self.rows, self.tile = spec
            (
                self.grad_in, self.carried_in, self.give, self.got, self.part, self.arrived, self.own,
                self.total, self.in_sem, self.give_sem, self.part_sem,
            ) = parts
            self.tiles = columns // self.tile
            self.items = chips * self.tiles
            self.held = held

        def fetch(self, k):
            there = lax.rem(chip + 1 + lax.div(k, self.tiles), chips)
            slot = lax.rem(k, SLOTS)
            copies = []
            for which in range(2):
                start = (there * 2 + which) * rows + self.row
                at = (0, pl.ds(pl.multiple_of(start, 16), self.rows), multiple(lax.rem(k, self.tiles), self.tile))
                for i, (array, into) in enumerate(((grad, self.grad_in), (carried, self.carried_in))):
                    copies.append(
                        pltpu.make_async_copy(
                            array.at[at], into.at[slot, which], self.in_sem.at[slot, 2 * which + i]
                        )
                    )
            return copies

        def start_fetch(self, k):
            for copy in self.fetch(k):
                copy.start()

        def outgoing(self, k, which):
            slot = lax.rem(k, SLOTS)
            return self.grad_in[slot, which].astype(f32) + self.carried_in[slot, which]

        def give_copy(self, k):
            slot = lax.rem(k, SLOTS)
            return remote(self.give.at[slot], self.got.at[k], self.give_sem.at[slot], self.give_sem.at[SLOTS + k], mate)

        def part_copy(self, k, step):
            return remote(
                self.part.at[k], self.arrived.at[k], self.part_sem.at[0, k], self.part_sem.at[1, k], across[step]
            )

        def first(self, k, send=True):
            for copy in self.fetch(k):
                copy.wait()

            @pl.when(k >= SLOTS)
            def _():
                self.give_copy(k - SLOTS).wait_send()

            self.give[lax.rem(k, SLOTS)] = self.outgoing(k, 1 - core).astype(bf16)
            if send:
                self.give_copy(k).start()

        def second(self, k, step, now=False):
            summed = self.outgoing(k, core)
            self.give_copy(k).wait_recv()
            summed += self.got[k].astype(f32)
            if step < chips - 1:
                self.part[k] = summed.astype(bf16)
                if now or not self.held:
                    self.part_copy(k, step).start()
            else:
                self.own[k - step * self.tiles] = summed

            @pl.when(k + SLOTS < self.items)
            def _():
                self.start_fetch(k + SLOTS)

        def run(self, step, begun=0):
            start, end = step * self.tiles + begun, (step + 1) * self.tiles
            if start >= end:
                return
            self.first(jnp.int32(start))

            def body(k, carry):
                self.first(k)
                self.second(k - 1, step)
                return carry

            lax.fori_loop(start + 1, end, body, 0)
            self.second(jnp.int32(end - 1), step)

        def update(self, t):
            at = (pl.ds(self.row, self.rows), multiple(t, self.tile))
            summed = self.own[t]
            for step in range(chips - 1):
                k = step * self.tiles + t
                self.part_copy(k, step).wait_recv()
                summed += self.arrived[k].astype(f32)
            average = mean(summed, n)
            moved = nesterov * new_momentum[at] + average
            updated = new_params[at] - outer_rate * (average + nesterov * moved)
            new_momentum[at] = moved
            new_params[at] = updated
            return updated.astype(bf16)

        def product(self, t, weights):
            self.total[...] += lax.dot_general(
                weights, probes[:, multiple(t, self.tile)], (((1,), (1,)), ((), ())),
                preferred_element_type=f32,
            )

        def drain(self):
            for k in range(max(0, self.items - SLOTS), self.items):
                self.give_copy(jnp.int32(k)).wait_send()
            for step in range(chips - 1):
                def body(k, carry, step=step):
                    self.part_copy(k, step).wait_send()
                    return carry

                lax.fori_loop(step * self.tiles, (step + 1) * self.tiles, body, 0)

    held = len(segments) > 1 and chips == 2
    parts = [Segment(s, b, held and i == 1) for i, (s, b) in enumerate(zip(segments, buffers))]
    main, late = parts[0], parts[-1]

    for k in range(min(OPENING, late.tiles)):
        late.start_fetch(jnp.int32(k))
    barrier = pltpu.get_barrier_semaphore()
    others = [(r, t) for r in range(n) for t in range(splits) if r or t]
    other = lambda r, t: {"replica": lax.rem(me + r, n), "tensor": lax.rem(mine + t, splits)}
    near = [mate] + across + beside if len(segments) > 1 else [other(r, t) for r, t in others]
    for peer in near:
        pl.semaphore_signal(barrier, inc=1, device_id=peer, device_id_type=MESH)
    is_right, is_left = here + 1 < n_fsdp, here >= 1
    right, left = {"fsdp": here + 1}, {"fsdp": here - 1}

    @pl.when(is_right)
    def _():
        pl.semaphore_signal(barrier, inc=1, device_id=right, device_id_type=MESH)

    @pl.when(is_left)
    def _():
        pl.semaphore_signal(barrier, inc=1, device_id=left, device_id_type=MESH)

    opening = min(OPENING, late.tiles)
    late.first(jnp.int32(0), send=False)
    if main is not late:
        main.start_fetch(jnp.int32(0))
    pl.semaphore_wait(barrier, len(near) + is_right.astype(jnp.int32) + is_left.astype(jnp.int32))

    half = height // 2
    half_at = lambda place: pl.ds(pl.multiple_of(place * height + core * half, half), half)
    own_probe = pltpu.make_async_copy(probe, probes.at[multiple(here, height), :], state_sem.at[2])

    def right_copy(s):
        block = here - s + 1
        src = probe.at[multiple(core, half), :] if s == 1 else probes.at[half_at(block), :]
        return remote(src, probes.at[half_at(block), :], right_send.at[s - 1], fetch_recv.at[block], right)

    def left_copy(s):
        block = here + s - 1
        src = probe.at[multiple(core, half), :] if s == 1 else probes.at[half_at(block), :]
        return remote(src, probes.at[half_at(block), :], left_send.at[s - 1], fetch_recv.at[block], left)

    def share_copy(block):
        place = half_at(block)
        return remote(probes.at[place, :], probes.at[place, :], share_send.at[block], share_recv.at[block], mate)

    def relay(s, act):
        @pl.when(is_right & (here - s + 1 >= 0))
        def _():
            act(right_copy(s))

        @pl.when(is_left & (here + s - 1 < n_fsdp))
        def _():
            act(left_copy(s))

    start = lambda copy: copy.start()
    wait_send = lambda copy: copy.wait_send()
    wait_recv = lambda copy: copy.wait_recv()

    def landed(s, act):
        @pl.when(here - s >= 0)
        def _():
            act(here - s, right_copy)

        @pl.when(here + s < n_fsdp)
        def _():
            act(here + s, left_copy)

    def land(s):
        def act(block, _):
            place = half_at(block)
            remote(
                probes.at[place, :], probes.at[place, :], right_send.at[0], fetch_recv.at[block], mate
            ).wait_recv()
            share_copy(block).start()

        landed(s, act)
        if s + 1 < n_fsdp:
            relay(s + 1, start)

    late.give_copy(jnp.int32(0)).start()
    for k in range(1, opening):
        late.first(jnp.int32(k))
    for k in range(opening):
        late.second(jnp.int32(k), 0, now=True)
    if n_fsdp > 1:
        relay(1, start)
    own_probe.start()
    if main is not late:
        for k in range(1, min(SLOTS, main.items)):
            main.start_fetch(jnp.int32(k))
    for k in range(opening, min(SLOTS, late.items)):
        late.start_fetch(jnp.int32(k))
    state = (
        pltpu.make_async_copy(params, new_params, state_sem.at[0]),
        pltpu.make_async_copy(momentum, new_momentum, state_sem.at[1]),
    )
    for step in range(chips - 1):
        for i, part in enumerate(parts):
            part.run(step, begun=opening if step == 0 and part is late else 0)
    for copy in state:
        copy.start()
    if n_fsdp > 1:
        land(1)
    for part in parts:
        part.run(chips - 1)
    if n_fsdp > 2:
        land(2)
    for copy in state:
        copy.wait()
    own_probe.wait()
    for part in parts:
        part.total[...] = jnp.zeros_like(part.total)

    first_products = max(1, (2 * main.tiles) // 3)

    def before(t, carry):
        main.got[t] = main.update(t)
        return carry

    lax.fori_loop(0, first_products, before, 0)
    for s in range(3, n_fsdp):
        land(s)
    for s in range(1, n_fsdp):
        landed(s, lambda block, _: share_copy(block).wait_recv())

    def backlog(t, carry):
        main.product(t, main.got[t])
        return carry

    lax.fori_loop(0, first_products, backlog, 0)

    def after(part):
        def body(t, carry):
            part.product(t, part.update(t))
            return carry

        return body

    batch = n_fsdp * height
    piece = batch // splits
    copies = []
    if len(parts) == 1:
        lax.fori_loop(first_products, main.tiles, after(main), 0)
    else:
        turn = max(first_products, main.tiles - 2)
        lax.fori_loop(first_products, turn, after(main), 0)
        lead = min(AHEAD, late.tiles - opening)
        if held:
            for k in range(opening, opening + lead):
                late.part_copy(jnp.int32(k), 0).start()
        lax.fori_loop(turn, main.tiles, after(main), 0)

        halves = []
        for i in range(splits - 1):
            early_out[i] = main.total[:, multiple(lax.rem(mine + 1 + i, splits), piece)].astype(bf16)
            copy = remote(early_out.at[i], early_in.at[i], early_send.at[i], early_recv.at[i], beside[i])
            copy.start()
            halves.append(copy)
        copies += halves

        def late_step(t, carry):
            if held:
                @pl.when(t + opening + lead < late.tiles)
                def _():
                    late.part_copy(t + opening + lead, 0).start()

            return after(late)(t, carry)

        middle = min(3, late.tiles)
        lax.fori_loop(0, middle, late_step, 0)
        summed = main.total[:, multiple(mine, piece)]
        for i, copy in enumerate(halves):
            copy.wait_recv()
            summed += early_in[i].astype(f32)
        block_at = lambda which: pl.ds(pl.multiple_of(which * rows, 16), main.rows)
        gathered[block_at(me), :] = summed.astype(bf16)

        def block_copy(which, slot, device):
            ref = gathered.at[block_at(which), :]
            return remote(ref, ref, block_send.at[slot], block_recv.at[slot], device)

        sends = [block_copy(me, s, across[s]) for s in range(chips - 1)]
        sends.append(block_copy(me, chips - 1, mate))
        for copy in sends:
            copy.start()
        lax.fori_loop(middle, late.tiles, late_step, 0)

    for t in range(splits):
        late_out[t] = late.total[:, multiple(lax.rem(mine + t, splits), piece)].astype(bf16)
    messages = [
        remote(
            late_out.at[t], late_in.at[r * splits + t],
            late_send.at[r * splits + t], late_recv.at[r * splits + t], other(r, t),
        )
        for r, t in others
    ]
    for copy in messages:
        copy.start()
    copies += messages
    if len(parts) > 1:
        for s in range(chips - 1):
            source = lax.rem(chip + chips - 1 - s, chips) * 2 + core
            sends[s].wait_recv()
            copy = block_copy(source, chips + s, mate)
            copy.start()
            sends.append(copy)
        copies += sends
    for part in parts:
        part.drain()
    for s in range(1, n_fsdp):
        relay(s, wait_send)
        landed(s, lambda block, _: share_copy(block).wait_send())
    for copy in messages:
        copy.wait_recv()
    for r in range(n):
        summed = jnp.zeros((late.rows, piece), f32)
        for t in range(splits):
            summed += (late_in[r * splits + t] if r or t else late_out[0]).astype(f32)
        source = lax.rem(me + n - r, n)
        gathered[pl.ds(pl.multiple_of(source * rows + late.row, 16), late.rows), :] = summed.astype(bf16)
    if len(parts) > 1:
        for copy in sends[chips - 1 :]:
            copy.wait_recv()
    for copy in copies:
        copy.wait_send()


def writer(params_in, momentum_in, gathered, params_out, momentum_out, probe_out, turned, sem):
    copies = [
        pltpu.make_async_copy(params_in, params_out, sem.at[0]),
        pltpu.make_async_copy(momentum_in, momentum_out, sem.at[1]),
    ]
    for priority, copy in enumerate(copies):
        copy.start(priority=priority)
    turned[...] = gathered[...].astype(f32).T.astype(bf16)
    last = pltpu.make_async_copy(turned, probe_out, sem.at[2])
    last.start()
    for copy in (*copies, last):
        copy.wait()


def per_device(pseudo_grad, compensation, params, momentum, probe):
    n = lax.axis_size("replica")
    n_fsdp = lax.axis_size("fsdp")
    splits = lax.axis_size("tensor")
    chips = n // 2
    rows, columns = params.shape
    height = probe.shape[0]
    batch = n_fsdp * height
    piece = batch // splits
    segments = segments_of(rows, columns)
    dma = pltpu.SemaphoreType.DMA
    anywhere = pl.BlockSpec(memory_space=pl.ANY)
    vmem = pl.BlockSpec(memory_space=pltpu.VMEM)
    scratch = []
    for _, high, tile in segments:
        tiles = columns // tile
        sends = max(1, chips - 1) * tiles
        scratch += [
            pltpu.VMEM((SLOTS, 2, high, tile), bf16),
            pltpu.VMEM((SLOTS, 2, high, tile), f32),
            pltpu.VMEM((SLOTS, high, tile), bf16),
            pltpu.VMEM((chips * tiles, high, tile), bf16),
            pltpu.VMEM((sends, high, tile), bf16),
            pltpu.VMEM((sends, high, tile), bf16),
            pltpu.VMEM((tiles, high, tile), f32),
            pltpu.VMEM((high, batch), f32),
            dma((SLOTS, 4)),
            dma((SLOTS + chips * tiles,)),
            dma((2, sends)),
        ]
    _, late, _ = segments[-1]
    early = segments[0][1]
    scratch += [
        pltpu.VMEM((batch, columns), bf16),
        pltpu.VMEM((splits, late, piece), bf16),
        pltpu.VMEM((n * splits, late, piece), bf16),
    ]
    if len(segments) > 1:
        scratch += [pltpu.VMEM((max(1, splits - 1), early, piece), bf16)] * 2
    links = max(1, n_fsdp)
    scratch += [dma((3,))] + [dma((links,))] * 5 + [dma((n * splits,))] * 2 + [dma((splits,))] * 2 + [dma((n,))] * 2
    full = pltpu.VMEM((rows, columns), f32)
    new_params, new_momentum, gathered = pl.pallas_call(
        functools.partial(kernel, (n, n_fsdp, splits, rows, columns, height, segments)),
        out_shape=(full, full, pltpu.VMEM((n * rows, piece), bf16)),
        in_specs=[anywhere] * 5,
        out_specs=[vmem] * 3,
        scratch_shapes=scratch,
        compiler_params=pltpu.CompilerParams(
            collective_id=0, has_side_effects=True, vmem_limit_bytes=46 * 1024 * 1024
        ),
    )(pseudo_grad, compensation, params, momentum, probe)
    full = jax.ShapeDtypeStruct((rows, columns), f32)
    return pl.pallas_call(
        writer,
        out_shape=(full, full, jax.ShapeDtypeStruct((piece, n * rows), bf16)),
        in_specs=[vmem] * 3,
        out_specs=[anywhere] * 3,
        scratch_shapes=[pltpu.VMEM((piece, n * rows), bf16), dma((3,))],
        compiler_params=pltpu.CompilerParams(vmem_limit_bytes=8 * 1024 * 1024),
    )(*(pltpu.with_memory_space_constraint(x, pltpu.VMEM) for x in (new_params, new_momentum, gathered)))


def solution(mesh):
    in_specs = (
        P("replica", "fsdp", "tensor"),
        P("replica", "fsdp", "tensor"),
        P(("fsdp", "replica"), "tensor"),
        P(("fsdp", "replica"), "tensor"),
        P("fsdp", "tensor"),
    )
    out_specs = (
        P(("fsdp", "replica"), "tensor"),
        P(("fsdp", "replica"), "tensor"),
        P("tensor", "fsdp"),
    )
    return jax.shard_map(
        per_device, mesh=mesh, in_specs=in_specs, out_specs=out_specs, check_vma=False
    )
```
